128 devices in a mesh: front: 8 (over y_hi, z), tile: 16 (over x, y_lo, core).
Axes of the slice: x: 4, y: 4 (y_hi: 2, y_lo: 2; y = y_hi * 2 + y_lo), z: 4, core: 2. Of those that a mesh axis runs over, the one named last changes fastest.
Arguments:
- lower_basis: bfloat16 [8, 16, 512, 1024], P('front', 'tile'), may hold values from -0.75 to 0.75
- lower_coeff: bfloat16 [8, 16, 512, 1024], P('front', 'tile'), may hold values from -0.75 to 0.75
- upper_basis: bfloat16 [8, 16, 512, 1024], P('front', 'tile'), may hold values from -0.75 to 0.75
- upper_coeff: bfloat16 [8, 16, 512, 1024], P('front', 'tile'), may hold values from -0.75 to 0.75
- lower_rank: int32 [8, 16, 32], P('front', 'tile'), may hold values from 1 to 32
- upper_rank: int32 [8, 16, 32], P('front', 'tile'), may hold values from 1 to 32
- child_half: int32 [8, 16], replicated, may hold values from 0 to 1
- owner_shift: int32 [2, 32], replicated, may hold values from 0 to 3
Outputs:
- parent_tiles: bfloat16 [8, 16, 8192, 512], P('front', 'tile')
The draws below stay inside these ranges and needn't reach their ends.
Inputs may be any that keep to these rules, and one draw needn't show every extreme that they name: `child_half`: 0 keeps a tile's index, 1 moves it by 16.
All inputs are finite; a program needn't handle non-finite values.
Results may differ from the reference program's by a relative error of at most 0.0062.
Values may be sent and summed in bfloat16 or wider, within the bound.
No kernel may reach another device: no remote copies, remote signals or barrier semaphores. Data moves between devices by JAX's collectives and lax.ppermute only.
A program may use at most 192 MiB of HBM per device.

```python
import jax
import jax.numpy as jnp
from jax import lax

B = 512
R = 32
KP = 32
K = 1024
NC = 16
PT = 32
FRONTS = 8
PARENTS = 2


def touch_ends(entries, own_key, smallest, top_value):
    dims = entries.shape
    index_at = [jax.random.randint(jax.random.fold_in(own_key, axis), (), 0, dims[axis]) for axis in range(len(dims))]
    entries = entries.at[tuple(index_at)].set(smallest)
    longest = dims.index(max(dims))
    index_at[longest] = (index_at[longest] + 1) % dims[longest]
    return entries.at[tuple(index_at)].set(top_value)


def steps_of(key, extent, pieces, low, largest):
    level = 1.0
    for dim, parts in pieces:
        heights = jax.random.uniform(jax.random.fold_in(jax.random.fold_in(key, 6), dim), (parts,), jnp.float32, low / len(pieces), largest / len(pieces))
        level = level * jnp.repeat(jnp.exp(heights), extent[dim] // parts).reshape((-1,) + (1,) * (len(extent) - 1 - dim))
    return level


def bell_draw(stream_key, extent, deviation, limit, cuts=(), kind=jnp.bfloat16):
    drawn = deviation * jax.random.normal(stream_key, extent, jnp.float32)
    if cuts:
        drawn = drawn * steps_of(stream_key, extent, cuts, -0.22, 0.18)
    return jnp.clip(drawn, -limit, limit).astype(kind)


def setup_inputs(seed: int = 0) -> dict:
    keys = jax.random.split(jax.random.key(seed), 9)
    lower_basis = bell_draw(keys[0], (FRONTS, NC, B, K), ((KP * R * R * B) ** -0.125), 0.75, ((0, 8), (1, 16)))
    lower_coeff = bell_draw(keys[1], (FRONTS, NC, B, K), ((KP * R * R * B) ** -0.125), 0.75, ((0, 8), (1, 16)))
    upper_basis = bell_draw(keys[2], (FRONTS, NC, B, K), ((KP * R * R * B) ** -0.125), 0.75, ((0, 8), (1, 16)))
    upper_coeff = bell_draw(keys[3], (FRONTS, NC, B, K), ((KP * R * R * B) ** -0.125), 0.75, ((0, 8), (1, 16)))
    lower_rank = touch_ends(jax.random.randint(keys[4], (FRONTS, NC, KP), 1, R + 1), jax.random.fold_in(keys[4], 1), 1, R).astype(jnp.int32)
    upper_rank = touch_ends(jax.random.randint(keys[5], (FRONTS, NC, KP), 1, R + 1), jax.random.fold_in(keys[5], 1), 1, R).astype(jnp.int32)
    child_half = touch_ends(jax.random.randint(keys[6], (FRONTS, NC), 0, 2), jax.random.fold_in(keys[6], 1), 0, 1).astype(jnp.int32)
    owner_shift = touch_ends(jax.random.randint(keys[7], (PARENTS, PT), 0, 4), jax.random.fold_in(keys[7], 1), 0, 3).astype(jnp.int32)
    return {"lower_basis": lower_basis, "lower_coeff": lower_coeff, "upper_basis": upper_basis, "upper_coeff": upper_coeff, "lower_rank": lower_rank, "upper_rank": upper_rank, "child_half": child_half, "owner_shift": owner_shift}


def masked(basis, ranks):
    keep = (jnp.arange(R, dtype=jnp.int32)[None, None, :] < ranks[:, :, None]).astype(jnp.float32)
    rows = basis.shape[0]
    return basis.astype(jnp.float32).reshape(rows, B, KP, R) * keep[:, None]


def front_tiles(lower_basis, lower_coeff, upper_basis, upper_coeff, lower_rank, upper_rank):
    lower_kept = masked(lower_basis, lower_rank)
    coeff_rows = lower_coeff.astype(jnp.float32).reshape(NC, B, KP, R)

    def column(packed):
        upper_one, coeff_one, col_ranks = packed
        upper_rows = upper_one.astype(jnp.float32).reshape(B, KP, R)
        upper_kept = masked(coeff_one[None], col_ranks[None])[0].reshape(B, KP * R)
        middle = jnp.einsum('ibkr,bks->ikrs', coeff_rows, upper_rows).astype(jnp.bfloat16)
        middle = lax.optimization_barrier(middle).astype(jnp.float32)
        widened = jnp.einsum('ibkr,ikrs->ibks', lower_kept, middle).astype(jnp.bfloat16)
        widened = lax.optimization_barrier(widened).astype(jnp.float32).reshape(NC, B, KP * R)
        return jnp.einsum('ibk,ck->ibc', widened, upper_kept).astype(jnp.bfloat16)

    return lax.map(column, (upper_basis, upper_coeff, upper_rank))


def reference(lower_basis, lower_coeff, upper_basis, upper_coeff, lower_rank, upper_rank, child_half, owner_shift):
    all_tiles = lax.map(lambda packed: front_tiles(*packed),
                        (lower_basis, lower_coeff, upper_basis, upper_coeff, lower_rank, upper_rank))
    half_rows = NC // 2
    col_ids = jnp.arange(NC, dtype=jnp.int32)[:, None]
    slot_ids = jnp.arange(NC, dtype=jnp.int32)[None, :]
    col_half = slot_ids // half_rows
    row_group = slot_ids % half_rows
    parent_col = col_ids + NC * col_half

    def receiver(out_front):
        parent = out_front // 4
        offset = out_front % 4
        shifts = lax.dynamic_index_in_dim(owner_shift, parent, 0, keepdims=False)
        parent_row = 4 * row_group + (offset - shifts[parent_col]) % 4
        child_row = parent_row % NC
        row_half = parent_row // NC
        assembled = jnp.zeros((NC, NC, B, B), jnp.float32)
        for sibling in range(4):
            child_front = 4 * parent + sibling
            tiles = lax.dynamic_index_in_dim(all_tiles, child_front, 0, keepdims=False)
            halves = lax.dynamic_index_in_dim(child_half, child_front, 0, keepdims=False)
            matches = (halves[col_ids] == col_half) & (halves[child_row] == row_half)
            picked = tiles[col_ids, child_row].astype(jnp.float32)
            assembled = assembled + jnp.where(matches[:, :, None, None], picked, jnp.float32(0.0))
        return assembled.astype(jnp.bfloat16).reshape(NC, NC * B, B)

    return lax.map(receiver, jnp.arange(FRONTS, dtype=jnp.int32))
```

```python
import functools

import jax
import jax.numpy as jnp
from jax import lax
from jax.experimental import pallas as pl
from jax.experimental.pallas import tpu as pltpu
from jax.sharding import PartitionSpec as P

B = 512
R = 32
KP = 32
K = KP * R
BF = jnp.bfloat16
F32 = jnp.float32
ORDER = (2, 1, 3, 0)


def lanes(rows):
    return lax.broadcasted_iota(jnp.int32, (rows, 128), 1)


def kept(ranks, first):
    lane = lanes(1)
    bound = jnp.zeros((1, 128), jnp.int32)
    for panel in range(4):
        bound = jnp.where(lane // R == panel, ranks[first + panel], bound)
    return jnp.where(lane % R < bound, 1.0, 0.0).astype(F32)


def pack_kernel(lower_rank, upper_rank, y_ref, p_ref, z_ref):
    first = 4 * pl.program_id(0)
    low = lanes(B) < 64
    y = y_ref[...].astype(F32) * kept(lower_rank, first)
    p = p_ref[...].astype(F32) * kept(upper_rank, first)
    z_ref[0] = jnp.where(low, y, pltpu.roll(p, 64, 1)).astype(BF)
    z_ref[1] = jnp.where(low, pltpu.roll(y, 64, 1), p).astype(BF)


def pack(lower_rank, upper_rank, y, p):
    return pl.pallas_call(
        pack_kernel,
        grid_spec=pltpu.PrefetchScalarGridSpec(
            num_scalar_prefetch=2,
            grid=(8,),
            in_specs=[pl.BlockSpec((B, 128), lambda e, *_: (0, e))] * 2,
            out_specs=pl.BlockSpec((2, B, 128), lambda e, *_: (e, 0, 0)),
        ),
        out_shape=jax.ShapeDtypeStruct((16, B, 128), BF),
    )(lower_rank, upper_rank, y, p)


def middle_kernel(z_ref, *refs):
    outs, p_all = refs[:4], refs[4]
    low = lanes(B) < 64
    for a in range(8):
        even = pltpu.roll(z_ref[2 * a].astype(F32), 64, 1)
        p_all[:, 128 * a : 128 * a + 128] = jnp.where(low, even, z_ref[2 * a + 1].astype(F32)).astype(BF)
    wide = lax.broadcasted_iota(jnp.int32, (R, K), 1)
    first = (wide // R) % 2 == 0
    low_m = lanes(R) < 64
    for a in range(8):
        odd = pltpu.roll(z_ref[2 * a + 1].astype(F32), 64, 1)
        y_pair = jnp.where(low, z_ref[2 * a].astype(F32), odd)
        prod = jnp.dot(y_pair.T.astype(BF), p_all[...], preferred_element_type=F32)
        one = jnp.where(first, prod[0:32], prod[32:64])
        two = jnp.where(first, prod[64:96], prod[96:128])
        for b in range(8):
            col = slice(128 * b, 128 * b + 128)
            group = (a // 2 - b // 2) % 4
            outs[group][2 * b, a % 2] = jnp.where(low_m, one[:, col], pltpu.roll(two[:, col], 64, 1)).astype(BF)
            outs[group][2 * b + 1, a % 2] = jnp.where(low_m, pltpu.roll(one[:, col], 64, 1), two[:, col]).astype(BF)


def middles(z):
    return pl.pallas_call(
        middle_kernel,
        out_shape=[jax.ShapeDtypeStruct((16, 2, R, 128), BF)] * 4,
        scratch_shapes=[pltpu.VMEM((B, K), BF)],
    )(z)


def owner_scalars(ids, child_half, owner_shift):
    front, tile = ids[0], ids[1]
    parent, place = front // 4, front % 4
    own_half = child_half[front, tile]
    shift = owner_shift[parent, tile + 16 * own_half]
    return place, shift, tile


def schur_kernel(ids, child_half, owner_shift, *refs):
    xs, r_ref, q_ref, outs = refs[:4], refs[4], refs[5], refs[6:10]
    x_s, w_s, o_s, in_sem, out_sem = refs[10:]
    place, shift, tile = owner_scalars(ids, child_half, owner_shift)
    my_y, my_h = (tile // 2) % 2, tile % 2
    for slot in range(4):
        residue = ((my_y + slot // 2) % 2) * 2 + (my_h + slot % 2) % 2
        away = (residue + shift - place + 8) % 4
        at = jnp.where(away == 2, 0, jnp.where(away == 0, 3, jnp.where(away == 1, 1, 2)))
        pltpu.make_async_copy(xs[slot], x_s.at[at], in_sem.at[at]).start()
    low_m = lanes(R) < 64
    row = lax.broadcasted_iota(jnp.int32, (256, 256), 0) // R
    diag = row == lax.broadcasted_iota(jnp.int32, (256, 256), 1) // R
    for at, away in enumerate(ORDER):
        residue = (place + away - shift + 4) % 4
        yy, hh = residue // 2, residue % 2
        pltpu.make_async_copy(xs[0], x_s.at[at], in_sem.at[at]).wait()
        for quad in range(4):
            parts = []
            for e in (2 * quad, 2 * quad + 1):
                one = r_ref[2 * e, yy].astype(F32)
                two = r_ref[2 * e + 1, yy].astype(F32)
                left = jnp.where(low_m, one, pltpu.roll(two, 64, 1))
                right = jnp.where(low_m, pltpu.roll(one, 64, 1), two)
                parts.append(jnp.where(hh == 0, left, right))
            compact = jnp.concatenate(parts, axis=1)
            block = jnp.where(diag, jnp.concatenate([compact] * 8, axis=0), 0.0).astype(BF)
            cols = slice(256 * quad, 256 * quad + 256)
            w_s[:, cols] = jnp.dot(x_s[at, :, cols], block, preferred_element_type=F32).astype(BF)
        o_s[at] = jnp.dot(w_s[...], q_ref[...], preferred_element_type=F32).astype(BF)
        pltpu.make_async_copy(o_s.at[at], outs[at], out_sem.at[at]).start()
    for at in range(4):
        pltpu.make_async_copy(o_s.at[at], outs[at], out_sem.at[at]).wait()


def schur(ids, child_half, owner_shift, xs, r, q_t):
    any_spec = pl.BlockSpec(memory_space=pl.ANY)
    vmem = pl.BlockSpec(memory_space=pltpu.VMEM)
    return pl.pallas_call(
        schur_kernel,
        grid_spec=pltpu.PrefetchScalarGridSpec(
            num_scalar_prefetch=3,
            grid=(),
            in_specs=[any_spec] * 4 + [vmem, vmem],
            out_specs=[any_spec] * 4,
            scratch_shapes=[
                pltpu.VMEM((4, B, K), BF),
                pltpu.VMEM((B, K), BF),
                pltpu.VMEM((4, B, B), BF),
                pltpu.SemaphoreType.DMA((4,)),
                pltpu.SemaphoreType.DMA((4,)),
            ],
        ),
        out_shape=[jax.ShapeDtypeStruct((B, B), BF)] * 4,
    )(ids, child_half, owner_shift, *xs, r, q_t)


def place_kernel(ids, child_half, owner_shift, *refs, apart):
    tiles, out = refs[:4], refs[-1]
    front, tile = ids[0], ids[1]
    parent, place = front // 4, front % 4
    row_x = (tile // 4 + apart) % 4
    slots = []
    for away in ORDER:
        child = 4 * parent + (place - away + 4) % 4
        col_half = child_half[child, tile]
        shift = owner_shift[parent, tile + 16 * col_half]
        row = 4 * row_x + (place - shift + 4) % 4
        slots.append(2 * col_half + child_half[child, row])
    values = [t[...].astype(F32) for t in tiles]
    for slot in range(4):
        total = jnp.where(slots[0] == slot, values[0], 0.0)
        for one in range(1, 4):
            total = total + jnp.where(slots[one] == slot, values[one], 0.0)
        out[slot, 0] = total.astype(BF)


def place_group(ids, child_half, owner_shift, tiles, out, apart):
    rows = 128
    extra = () if out is None else (out,)
    return pl.pallas_call(
        functools.partial(place_kernel, apart=apart),
        grid_spec=pltpu.PrefetchScalarGridSpec(
            num_scalar_prefetch=3,
            grid=(B // rows,),
            in_specs=[pl.BlockSpec((rows, B), lambda r, *_: (r, 0))] * 4
            + [pl.BlockSpec(memory_space=pl.ANY)] * len(extra),
            out_specs=pl.BlockSpec(
                (4, 1, rows, B), lambda r, ids, *_: (0, (ids[1] // 4 + apart) % 4, r, 0)
            ),
        ),
        out_shape=jax.ShapeDtypeStruct((4, 4, B, B), BF),
        input_output_aliases={} if out is None else {7: 0},
    )(ids, child_half, owner_shift, *tiles, *extra)


def tile_pairs(move):
    return [(t, move(t)) for t in range(16)]


def over_x(block, step):
    return lax.ppermute(block, "tile", tile_pairs(lambda t: (((t >> 2) + step) % 4) << 2 | (t & 3)))


def over_y(block):
    return lax.ppermute(block, "tile", tile_pairs(lambda t: t ^ 2))


def over_core(block):
    return lax.ppermute(block, "tile", tile_pairs(lambda t: t ^ 1))


def over_z(block, step):
    return lax.ppermute(block, "front", [(f, (f & 4) | ((f + step) & 3)) for f in range(8)])


def per_device(
    lower_basis, lower_coeff, upper_basis, upper_coeff, lower_rank, upper_rank, child_half, owner_shift
):
    ids = jnp.stack([lax.axis_index("front"), lax.axis_index("tile")]).astype(jnp.int32)
    table = (ids, child_half, owner_shift)
    own = lower_basis[0, 0]
    packed = pack(lower_rank[0, 0], upper_rank[0, 0], lower_coeff[0, 0], upper_basis[0, 0])
    gathered = lax.all_to_all(packed, "tile", 0, 0, tiled=True)
    gathered, own = lax.optimization_barrier((gathered, own))
    mids = middles(gathered)
    q_t = upper_coeff[0, 0].T
    beside = over_y(own)
    near = {0: own, 1: over_x(own, -1), 3: over_x(own, 1), 2: over_x(own, 2)}
    far = {0: beside, 1: over_y(near[1]), 3: over_x(beside, 1), 2: over_y(near[2])}
    out = None
    for apart in (0, 1, 3, 2):
        mine = lax.all_to_all(mids[apart], "tile", 0, 0, tiled=True)
        xs = (near[apart], over_core(near[apart]), far[apart], over_core(far[apart]))
        tiles = schur(*table, xs, mine, q_t)
        moved = [over_z(tiles[at], ORDER[at]) for at in range(3)] + [tiles[3]]
        out = place_group(*table, moved, out, apart)
    return out.reshape(1, 1, 16 * B, B)


def solution(mesh):
    shard = P("front", "tile", None, None)
    ranks = P("front", "tile", None)
    return jax.shard_map(
        per_device,
        mesh=mesh,
        in_specs=(shard, shard, shard, shard, ranks, ranks, P(), P()),
        out_specs=shard,
        check_vma=False,
    )
```
